16 devices in a mesh: rep: 4 (over y, z, core), dp: 4 (over x).
Axes of the slice: x: 4, y: 2, z: 1, core: 2. Of those that a mesh axis runs over, the one named last changes fastest.
The devices are a block of a 4x4x8 slice.
Arguments:
- x: bfloat16 [16, 4096, 768], P(('rep', 'dp')), parts along dimension 0
- dy: bfloat16 [16, 4096, 768], P(('rep', 'dp')), parts along dimension 0
- w_gate: bfloat16 [2, 768, 1792], replicated
- w_up: bfloat16 [2, 768, 1792], replicated
- w_down: bfloat16 [2, 1792, 768], replicated
- m_w_gate: float32 [2, 768, 1792], replicated
- m_w_up: float32 [2, 768, 1792], replicated
- m_w_down: float32 [2, 1792, 768], replicated
- v_w_gate: float32 [2, 768, 1792], replicated
- v_w_up: float32 [2, 768, 1792], replicated
- v_w_down: float32 [2, 1792, 768], replicated
Outputs:
- output 1: bfloat16 [8, 768, 1792], P('rep'), parts along dimension 0
- output 2: bfloat16 [8, 768, 1792], P('rep'), parts along dimension 0
- output 3: bfloat16 [8, 1792, 768], P('rep'), parts along dimension 0
- output 4: float32 [8, 768, 1792], P('rep'), parts along dimension 0
- output 5: float32 [8, 768, 1792], P('rep'), parts along dimension 0
- output 6: float32 [8, 1792, 768], P('rep'), parts along dimension 0
- output 7: float32 [8, 768, 1792], P('rep'), parts along dimension 0
- output 8: float32 [8, 768, 1792], P('rep'), parts along dimension 0
- output 9: float32 [8, 1792, 768], P('rep'), parts along dimension 0
There are 4 independent parts. The reference program is written for one: setup_inputs(seed, part) draws one part's arguments, and reference() takes and returns one part's arrays. A program takes and returns all parts, laid end to end along the dimension named above; an argument that names none is the same for every part.
All inputs are finite; a program needn't handle non-finite values.
Results may differ from the reference program's by a relative error of at most 0.022.
Values are sent between devices in bfloat16 or wider.
A program may use at most 768 MiB of HBM per device.

```python
import jax
import jax.numpy as jnp
from jax import lax

SEQUENCES = 4
TOKENS = 4096
D = 768
FF = 1792
LAYERS = 2
NAMES = ("w_gate", "w_up", "w_down")
SHAPES = {"w_gate": (LAYERS, D, FF), "w_up": (LAYERS, D, FF), "w_down": (LAYERS, FF, D)}


def bump(key, n, height):
    away = (jnp.arange(n, dtype=jnp.int32) - jax.random.randint(key, (), 0, n, jnp.int32)) % n
    return jnp.where(away < n // 8, height, 1.0)


def together(key, own, strength):
    shared = jax.random.normal(key, own.shape[1:], jnp.float32)
    return (own + strength * shared) * lax.rsqrt(1 + strength * strength)


def setup_inputs(seed: int = 0, part: int = 0) -> dict:
    kx, kdy, ka, kb, kz, kf, kh, kl, *keys = jax.random.split(jax.random.key(seed), 8 + 3 * len(NAMES))
    kx, kdy, ka, kb = (jax.random.fold_in(k, part) for k in (kx, kdy, ka, kb))
    kw, km, kv = (keys[i::3] for i in range(3))
    shape = (SEQUENCES, TOKENS, D)
    much_x, much_dy = jax.random.uniform(kz, (2,), jnp.float32, 0.0, 1.0)
    loud = 2.0 ** jax.random.uniform(jax.random.fold_in(kz, 1), (), jnp.float32, -1.0, 2.0)
    layers = 2.0 ** jax.random.uniform(kl, (LAYERS, 1, 1), jnp.float32, -1.0, 1.0)
    x = together(ka, jax.random.normal(kx, shape, jnp.float32), much_x) * bump(kf, D, 4.0)
    dy = together(kb, jax.random.normal(kdy, shape, jnp.float32), much_dy)
    drawn = {"x": x.astype(jnp.bfloat16), "dy": (loud * dy * (SEQUENCES * TOKENS) ** -0.5).astype(jnp.bfloat16)}
    for key, name in zip(kw, NAMES, strict=True):
        w = jax.random.normal(key, SHAPES[name], jnp.float32) * SHAPES[name][1] ** -0.5
        drawn[name] = (w * {"w_gate": 1.0, "w_up": bump(kh, FF, 4.0), "w_down": layers}[name]).astype(jnp.bfloat16)
    for key, name in zip(km, NAMES, strict=True):
        drawn[f"m_{name}"] = 0.1 * jax.random.normal(key, SHAPES[name], jnp.float32)
    for key, name in zip(kv, NAMES, strict=True):
        drawn[f"v_{name}"] = jax.random.uniform(key, SHAPES[name], jnp.float32, 0.005, 0.015)
    return drawn


def matmul(a, w):
    return jnp.dot(a, w, preferred_element_type=jnp.float32).astype(jnp.bfloat16)


def normed(h):
    wide = h.astype(jnp.float32)
    scale = lax.rsqrt(jnp.mean(wide**2, -1, keepdims=True) + 1e-6)
    return (wide * scale).astype(jnp.bfloat16)


def layer(h, w):
    a = normed(h)
    gate = jnp.dot(a, w["w_gate"], preferred_element_type=jnp.float32)
    up = jnp.dot(a, w["w_up"], preferred_element_type=jnp.float32)
    return h + matmul((jax.nn.silu(gate) * up).astype(jnp.bfloat16), w["w_down"])


def adamw(w, m, v, g):
    m = 0.9 * m + 0.1 * g
    v = 0.95 * v + 0.05 * g * g
    step = m * lax.rsqrt(v + 1e-8) + 0.1 * w
    return (w - 0.02 * step).astype(jnp.bfloat16), m, v


def clipped(gradients, sum_of_squares, count):
    factor = jnp.minimum(1.0, 0.5 * lax.rsqrt(sum_of_squares / count + 1e-30))
    return [g * factor for g in gradients]


def stack(weights, h):
    return lax.scan(lambda h, w: (layer(h, w), None), h, weights)[0]


def reference(x, dy, w_gate, w_up, w_down, m_w_gate, m_w_up, m_w_down, v_w_gate, v_w_up, v_w_down):
    weights = dict(zip(NAMES, (w_gate, w_up, w_down), strict=True))

    def take(so_far, sequence):
        h, by_y = sequence
        _, back = jax.vjp(lambda w: stack(w, h), weights)
        return jax.tree.map(lambda total, term: total + term.astype(jnp.float32), so_far, back(by_y)[0]), None

    none_yet = {name: jnp.zeros(w.shape, jnp.float32) for name, w in weights.items()}
    by_weights, _ = lax.scan(take, none_yet, (x, dy))
    gradients = [by_weights[name].astype(jnp.bfloat16).astype(jnp.float32) for name in NAMES]
    gradients = clipped(gradients, sum(jnp.sum(g * g) for g in gradients), sum(g.size for g in gradients))
    new = [
        adamw(w.astype(jnp.float32), m, v, g)
        for w, m, v, g in zip((w_gate, w_up, w_down), (m_w_gate, m_w_up, m_w_down), (v_w_gate, v_w_up, v_w_down), gradients, strict=True)
    ]
    return tuple(one[which] for which in range(3) for one in new)
```

```python
import functools

import jax
import jax.numpy as jnp
from jax import lax
from jax.experimental import pallas as pl
from jax.experimental.pallas import tpu as pltpu
from jax.sharding import PartitionSpec as P


F32, BF16 = jnp.float32, jnp.bfloat16
TILE = 512
SUB = 512
UNIT = 256
FULL_VMEM = 60 << 20
PIECES = {1: (2, 2, 3), 0: (3, 3, 1)}


def params(**kw):
    return pltpu.CompilerParams(vmem_limit_bytes=FULL_VMEM, **kw)


def cost(matmuls, moved, tokens, d, width):
    return pl.CostEstimate(flops=2 * matmuls * tokens * d * width, bytes_accessed=moved, transcendentals=0)


def dot(a, b, ca, cb):
    return lax.dot_general(a, b, (((ca,), (cb,)), ((), ())), preferred_element_type=F32)


def scale_of(wide):
    return lax.rsqrt(jnp.mean(wide * wide, -1, keepdims=True) + 1e-6)


def forward_kernel(x_ref, wg_ref, wu_ref, wd_ref, a_ref, h_ref, b_ref, gate_ref, up_ref, p_ref):
    rows = SUB
    for sub in range(x_ref.shape[0] // SUB):
        at = slice(sub * rows, (sub + 1) * rows)
        x = x_ref[at, :].astype(F32)
        a = (x * scale_of(x)).astype(BF16)
        a_ref[at, :] = a
        for j in range(p_ref.shape[1] // UNIT):
            cols = slice(j * UNIT, (j + 1) * UNIT)
            gate = dot(a, wg_ref[:, cols], 1, 0)
            up = dot(a, wu_ref[:, cols], 1, 0)
            gate_ref[at, cols] = gate
            up_ref[at, cols] = up
            p_ref[at, cols] = (gate * jax.nn.sigmoid(gate) * up).astype(BF16)
    for sub in range(x_ref.shape[0] // SUB):
        at = slice(sub * rows, (sub + 1) * rows)
        h = x_ref[at, :] + dot(p_ref[at, :], wd_ref[...], 1, 0).astype(BF16)
        h_ref[at, :] = h
        wide = h.astype(F32)
        b_ref[at, :] = (wide * scale_of(wide)).astype(BF16)


def forward(x, wg, wu, wd, layer):
    tokens, d = x.shape
    ff = wg.shape[2]
    rows = pl.BlockSpec((TILE, d), lambda t: (t, 0))
    hidden = pl.BlockSpec((TILE, ff), lambda t: (t, 0))
    whole = lambda r, c: pl.BlockSpec((None, r, c), lambda t: (layer, 0, 0), pipeline_mode=pl.Buffered(1))
    out = jax.ShapeDtypeStruct((tokens, d), BF16)
    wide = jax.ShapeDtypeStruct((tokens, ff), F32)
    return pl.pallas_call(
        forward_kernel,
        grid=(tokens // TILE,),
        in_specs=[rows, whole(d, ff), whole(d, ff), whole(ff, d)],
        out_specs=[rows] * 3 + [hidden] * 2,
        out_shape=[out] * 3 + [wide] * 2,
        scratch_shapes=[pltpu.VMEM((TILE, ff), BF16)],
        compiler_params=params(dimension_semantics=("arbitrary",)),
        cost_estimate=cost(3, 8 * tokens * d + 6 * d * ff, tokens, d, ff),
        name="forward",
    )(x, wg, wu, wd)


def remote(src, dst, sems, i, to):
    send, recv = sems
    return pltpu.make_async_remote_copy(
        src_ref=src, dst_ref=dst, send_sem=send.at[i], recv_sem=recv.at[i], device_id={"dp": to}, device_id_type=pl.DeviceIdType.MESH
    )


def around(n):
    me = lax.axis_index("dp")
    return lax.rem(me + 1, n), lax.rem(me + n - 1, n)


class Sum:
    def __init__(self, parts, n, middle):
        self.operands, self.n, self.middle = list(parts), n, middle
        half = parts[0].shape[1:]
        self.half = half
        self.outs = [jax.ShapeDtypeStruct((2, *half), BF16), jax.ShapeDtypeStruct((8, half[-1]), F32)]
        self.out_specs = [pl.BlockSpec((2, *half), lambda t: (0,) * 4), pl.BlockSpec((8, half[-1]), lambda t: (0, 0))]
        self.scratch = [pltpu.VMEM((k, *half), BF16) for k in (2, 2, 4, 2, 2)]
        self.scratch += [pltpu.SemaphoreType.DMA((6,)), pltpu.SemaphoreType.DMA((6,)), pltpu.SemaphoreType.DMA((1,))]

    def bind(self, refs):
        to_right, to_left, rest, self.share, self.squares, self.from_left, self.from_right, self.rest, self.sums, self.second, *sems, local = refs
        right, left = around(self.n)
        self.copies = [
            remote(to_right.at[0], self.from_left.at[0], sems, 0, right),
            remote(to_left.at[0], self.from_right.at[0], sems, 1, left),
            remote(to_right.at[1], self.from_left.at[1], sems, 2, right),
            remote(to_left.at[1], self.from_right.at[1], sems, 3, left),
            remote(self.sums.at[0], self.second.at[0], sems, 4, right),
            remote(self.sums.at[1], self.second.at[1], sems, 5, left),
        ]
        self.local = pltpu.make_async_copy(rest, self.rest, local.at[0])

    def start(self):
        self.local.start()
        for copy in self.copies[:4]:
            copy.start()

    def step(self):
        self.local.wait()
        for i, came in enumerate((self.from_left, self.from_right)):
            self.copies[i].wait_recv()

            @pl.loop(0, self.half[0])
            def _(k):
                self.sums[i, k] = (self.rest[i, k].astype(F32) + came[0, k].astype(F32)).astype(BF16)

            self.copies[4 + i].start()

    def end(self):
        for copy in self.copies[2:]:
            copy.wait_recv()
        self.squares[...] = jnp.zeros_like(self.squares)
        for i, came in enumerate((self.from_right, self.from_left)):

            @pl.loop(0, self.half[0])
            def _(k):
                whole = self.rest[2 + i, k].astype(F32) + came[1, k].astype(F32) + self.second[i, k].astype(F32)
                self.share[i, k] = whole.astype(BF16)
                rounded = whole.astype(BF16).astype(F32)
                self.squares[...] += jnp.sum((rounded * rounded).reshape(-1, 8, rounded.shape[-1]), 0)

        for copy in self.copies:
            copy.wait_send()


class Gather:
    def __init__(self, share, n, middle):
        self.operands, self.n, self.middle = [share], n, middle
        self.outs = [jax.ShapeDtypeStruct(share.shape, BF16)] * 3
        self.out_specs = [pl.BlockSpec(memory_space=pl.ANY)] * 3
        self.scratch = [pltpu.SemaphoreType.DMA((6,)), pltpu.SemaphoreType.DMA((6,))]

    def bind(self, refs):
        share, after, far, before, *sems = refs
        right, left = around(self.n)
        self.copies = [
            remote(share.at[0], before.at[0], sems, 0, right),
            remote(share.at[1], after.at[1], sems, 1, left),
            remote(share.at[1], before.at[1], sems, 2, right),
            remote(share.at[0], after.at[0], sems, 3, left),
            remote(before.at[0], far.at[0], sems, 4, right),
            remote(after.at[1], far.at[1], sems, 5, left),
        ]

    def start(self):
        for copy in self.copies[:4]:
            copy.start()

    def step(self):
        for i in range(2):
            self.copies[i].wait_recv()
            self.copies[4 + i].start()

    def end(self):
        for copy in self.copies[2:]:
            copy.wait_recv()
        for copy in self.copies:
            copy.wait_send()


def run(body, n, steps, ins, in_specs, outs, out_specs, scratch, tasks, number, **kw):
    groups = [(ins, outs, scratch), *((t.operands, t.outs, t.scratch) for t in tasks)]

    def kernel(*refs):
        at, dealt = 0, [[] for _ in groups]
        for which in range(3):
            for i, group in enumerate(groups):
                dealt[i] += refs[at : at + len(group[which])]
                at += len(group[which])
        t = pl.program_id(0)
        for task, own in zip(tasks, dealt[1:], strict=True):
            task.bind(own)
        if tasks:

            @pl.when(t == 0)
            def _():
                barrier = pltpu.get_barrier_semaphore()
                for to in around(n):
                    pl.semaphore_signal(barrier, inc=1, device_id={"dp": to}, device_id_type=pl.DeviceIdType.MESH)
                pl.semaphore_wait(barrier, 2)
                for task in tasks:
                    task.start()

            for task in tasks:
                pl.when(t == task.middle)(task.step)
        body(*dealt[0])
        for task in tasks:
            pl.when(t == steps - 1)(task.end)

    anywhere = pl.BlockSpec(memory_space=pl.ANY)
    out = pl.pallas_call(
        kernel,
        grid=(steps,),
        in_specs=list(in_specs) + [anywhere for t in tasks for _ in t.operands],
        out_specs=list(out_specs) + [s for t in tasks for s in t.out_specs],
        out_shape=list(outs) + [o for t in tasks for o in t.outs],
        scratch_shapes=list(scratch) + [s for t in tasks for s in t.scratch],
        compiler_params=params(
            dimension_semantics=("arbitrary",), **(dict(collective_id=number, has_side_effects=True) if tasks else {})
        ),
        **kw,
    )(*ins, *(o for t in tasks for o in t.operands))
    out, given = list(out), []
    own, out = out[: len(outs)], out[len(outs) :]
    for t in tasks:
        given.append(out[: len(t.outs)])
        out = out[len(t.outs) :]
    return own, *given


def piece_kernel(units, start, n, saved, a_ref, dy_ref, *refs):
    if saved:
        gate_ref, up_ref, wd_ref, to_right, to_left, rest, acc, acc_d, p_s, dgu_ref = refs
    else:
        wg_ref, wu_ref, wd_ref, to_right, to_left, rest, dgu_ref, acc, acc_d, p_s = refs
    width = units * UNIT
    t = pl.program_id(0)

    @pl.when(t == 0)
    def _():
        acc[...] = jnp.zeros_like(acc)
        acc_d[...] = jnp.zeros_like(acc_d)

    def accumulate(j, sub):
        at = slice(sub * SUB, (sub + 1) * SUB)
        cols = slice(j * UNIT, (j + 1) * UNIT)
        ups = slice(width + j * UNIT, width + (j + 1) * UNIT)
        acc[:, cols] += dot(a_ref[at, :], dgu_ref[at, cols], 0, 0)
        acc[:, ups] += dot(a_ref[at, :], dgu_ref[at, ups], 0, 0)
        acc_d[cols, :] += dot(p_s[at, cols], dy_ref[at, :], 0, 0)

    before = None
    for sub in range(a_ref.shape[0] // SUB):
        for j in range(units):
            at = slice(sub * SUB, (sub + 1) * SUB)
            cols = slice(j * UNIT, (j + 1) * UNIT)
            there = slice((start + j) * UNIT, (start + j + 1) * UNIT)
            gate = gate_ref[at, there] if saved else dot(a_ref[at, :], wg_ref[:, there], 1, 0)
            up = up_ref[at, there] if saved else dot(a_ref[at, :], wu_ref[:, there], 1, 0)
            dp = dot(dy_ref[at, :], wd_ref[there, :], 1, 1).astype(BF16).astype(F32)
            s = jax.nn.sigmoid(gate)
            act = gate * s
            p_s[at, cols] = (act * up).astype(BF16)
            dgu_ref[at, width + j * UNIT : width + (j + 1) * UNIT] = (dp * act).astype(BF16)
            dgu_ref[at, cols] = (dp * up * (s * (1.0 + gate * (1.0 - s)))).astype(BF16)
            if before:
                accumulate(*before)
            before = j, sub
    accumulate(*before)

    @pl.when(t == pl.num_programs(0) - 1)
    def _():
        part = to_right.shape[2]
        small = UNIT // (2 * n)
        me = lax.axis_index("dp")

        def put(ref, by, half):
            at = (lax.rem(me + by, n) * 2 + half)
            rows = pl.ds(pl.multiple_of(at * part, part), part)
            for u in range(units):
                for which in range(2):
                    low = which * width + u * UNIT
                    ref[3 * u + which] = acc[rows, low : low + UNIT].astype(BF16)
                thin = pl.ds(pl.multiple_of(u * UNIT + at * small, small), small)
                for b in range(part // small):
                    ref[3 * u + 2, b * small : (b + 1) * small, :] = acc_d[thin, b * UNIT : (b + 1) * UNIT].astype(BF16)

        put(to_right.at[0], 2, 0)
        put(to_right.at[1], 1, 1)
        put(to_left.at[0], 2, 1)
        put(to_left.at[1], n - 1, 0)
        put(rest.at[0], 1, 0)
        put(rest.at[1], n - 1, 1)
        put(rest.at[2], 0, 0)
        put(rest.at[3], 0, 1)


def piece(a, dy, weights, saved, layer, start, units, n, tasks=(), number=0):
    tokens, d = a.shape
    width = units * UNIT
    tile = TILE
    rows = pl.BlockSpec((tile, d), lambda t: (t, 0))
    part = d // (2 * n)
    cols = pl.BlockSpec((None, d, weights[0].shape[2]), lambda t: (layer, 0, 0), pipeline_mode=pl.Buffered(1))
    down = pl.BlockSpec((None, weights[0].shape[2], d), lambda t: (layer, 0, 0), pipeline_mode=pl.Buffered(1))
    kept = pl.BlockSpec((tile, weights[0].shape[2]), lambda t: (t, 0))
    both = pl.BlockSpec((tile, 2 * width), lambda t: (t, 0))
    shapes = [(2, 3 * units, part, UNIT)] * 2 + [(4, 3 * units, part, UNIT)]
    outs = [jax.ShapeDtypeStruct(s, BF16) for s in shapes]
    specs = [pl.BlockSpec(s, lambda t: (0,) * 4) for s in shapes]
    scratch = [pltpu.VMEM((d, 2 * width), F32), pltpu.VMEM((width, d), F32), pltpu.VMEM((tile, width), BF16)]
    if saved:
        ins, operands = [kept, kept], saved
        scratch.append(pltpu.VMEM((tile, 2 * width), BF16))
    else:
        ins, operands = [cols, cols], weights[:2]
        outs.append(jax.ShapeDtypeStruct((tokens, 2 * width), BF16))
        specs.append(both)
    return run(
        functools.partial(piece_kernel, units, start, n, bool(saved)),
        n,
        tokens // tile,
        (a, dy, *operands, weights[2]),
        [rows, rows] + ins + [down],
        outs,
        specs,
        scratch,
        tasks,
        number,
        cost_estimate=cost(4 if saved else 6, 4 * tokens * d + 12 * d * width, tokens, d, width),
        name=f"piece_{layer}_{start}",
    )


def back_kernel(count, *refs):
    parts = refs[:count]
    wg_ref, wu_ref, h_ref, dy_ref, out_ref = refs[count:]

    rows = SUB
    for sub in range(h_ref.shape[0] // SUB):
        span = slice(sub * rows, (sub + 1) * rows)

        def back(which, w_ref):
            total, at = None, 0
            for part in parts:
                width = part.shape[1] // 2
                term = dot(part[span, which * width : (which + 1) * width], w_ref[:, at : at + width], 1, 1)
                total, at = term if total is None else total + term, at + width
            return total.astype(BF16)

        da = (back(0, wg_ref) + back(1, wu_ref)).astype(F32)
        h = h_ref[span, :].astype(F32)
        scale = scale_of(h)
        along = jnp.mean(da * h, -1, keepdims=True)
        out_ref[span, :] = dy_ref[span, :] + (da * scale - h * (scale * scale * scale * along)).astype(BF16)


def back(parts, wg, wu, h, dy, layer, n, tasks=(), number=0):
    tokens, d = h.shape
    ff = wg.shape[2]
    rows = pl.BlockSpec((TILE, d), lambda t: (t, 0))
    whole = pl.BlockSpec((None, d, ff), lambda t: (layer, 0, 0), pipeline_mode=pl.Buffered(1))
    hidden = [pl.BlockSpec((TILE, g.shape[1]), lambda t: (t, 0)) for g in parts]
    return run(
        functools.partial(back_kernel, len(parts)),
        n,
        tokens // TILE,
        (*parts, wg, wu, h, dy),
        hidden + [whole, whole, rows, rows],
        [jax.ShapeDtypeStruct((tokens, d), BF16)],
        [rows],
        (),
        tasks,
        number,
        cost_estimate=cost(2, 6 * tokens * d + 4 * d * ff + 4 * tokens * ff, tokens, d, ff),
        name="back",
    )


class Finish(Sum):
    def __init__(self, parts, n, others, count):
        super().__init__(parts, n, 0)
        self.operands, self.count, self.others = self.operands + list(others), count, len(others)
        tile = (8, others[0].shape[1])
        self.outs.append(jax.ShapeDtypeStruct(tile, F32))
        self.out_specs.append(pl.BlockSpec(tile, lambda t: (0, 0)))
        self.scratch += [pltpu.VMEM((n, *tile), F32), pltpu.VMEM((len(others), *tile), F32), pltpu.SemaphoreType.DMA((1,))]
        self.scratch += [pltpu.SemaphoreType.DMA((n,)), pltpu.SemaphoreType.DMA((n,))]


def finish_kernel(task, refs):
    k = task.others
    parts, others, share, squares, factor = refs[:3], refs[3 : 3 + k], refs[3 + k], refs[4 + k], refs[5 + k]
    rest = refs[6 + k :]
    terms, held, local, send, recv = rest[8:]
    n = task.n
    me = lax.axis_index("dp")
    barrier = pltpu.get_barrier_semaphore()
    for by in range(1, n):
        pl.semaphore_signal(barrier, inc=1, device_id={"dp": lax.rem(me + by, n)}, device_id_type=pl.DeviceIdType.MESH)
    pl.semaphore_wait(barrier, n - 1)
    task.bind([*parts, share, squares, *rest[:8]])
    task.start()
    for i, other in enumerate(others):
        copy = pltpu.make_async_copy(other, held.at[i], local.at[0])
        copy.start()
        copy.wait()
    task.step()
    task.end()
    total = squares[...]
    for i in range(k):
        total += held[i]
    terms[me] = total
    copies = [remote(terms.at[me], terms.at[me], (send, recv), by, lax.rem(me + by, n)) for by in range(1, n)]
    for copy in copies:
        copy.start()
    for by in range(1, n):
        sender = lax.rem(me + n - by, n)
        remote(terms.at[sender], terms.at[sender], (send, recv), by, lax.rem(me + by, n)).wait_recv()
    everything = terms[0]
    for i in range(1, n):
        everything += terms[i]
    everything = jnp.sum(jnp.sum(everything, 0, keepdims=True), 1, keepdims=True)
    factor[...] = jnp.broadcast_to(jnp.minimum(1.0, 0.5 * lax.rsqrt(everything / task.count + 1e-30)), factor.shape)
    for copy in copies:
        copy.wait_send()


def finish(parts, n, others, count, number):
    task = Finish(parts, n, others, count)
    anywhere = pl.BlockSpec(memory_space=pl.ANY)
    return pl.pallas_call(
        lambda *refs: finish_kernel(task, refs),
        grid=(1,),
        in_specs=[anywhere] * len(task.operands),
        out_specs=task.out_specs,
        out_shape=task.outs,
        scratch_shapes=task.scratch,
        compiler_params=params(collective_id=number, has_side_effects=True),
        cost_estimate=pl.CostEstimate(flops=4 * 10**9, bytes_accessed=10**6, transcendentals=0),
        name="finish",
    )(*task.operands)


def adamw_kernel(n, count, me_ref, factor_ref, *refs):
    grads, ins, outs = refs[:count], refs[count : count + 9], refs[-9:]
    factor = factor_ref[0:1, 0:1]
    me = me_ref[0]
    for number in range(2 * n):
        at = lax.rem(me + number // 2, n) * 2 + number % 2
        ref = grads[number // 2].at[number % 2] if count == n else grads[number]
        for which in range(3):
            w_ref, m_ref, v_ref = (ins[which + 3 * i] for i in range(3))
            w_out, m_out, v_out = (outs[which + 3 * i] for i in range(3))
            part = ref.shape[1]
            if which < 2:
                spots = [((pl.ds(pl.multiple_of(at * part, part), part), slice(None)), ref[which])]
            else:
                small = w_ref.shape[0] // (2 * n)
                spots = [
                    ((pl.ds(pl.multiple_of(at * small, small), small), slice(b * UNIT, (b + 1) * UNIT)), ref[which, b * small : (b + 1) * small])
                    for b in range(part // small)
                ]
            for spot, g in spots:
                g = g.astype(F32) * factor
                m = 0.9 * m_ref[spot] + 0.1 * g
                v = 0.95 * v_ref[spot] + 0.05 * g * g
                w = w_ref[spot].astype(F32)
                m_out[spot] = m
                v_out[spot] = v
                w_out[spot] = (w - 0.02 * (m * lax.rsqrt(v + 1e-8) + 0.1 * w)).astype(BF16)


def adamw(arrays, done, grads, me, factor, layer, start, n):
    d = arrays[0].shape[1]
    units = grads[0].shape[-3] // 3
    wide = pl.BlockSpec((None, d, UNIT), lambda s, me: (layer, 0, start + s))
    tall = pl.BlockSpec((None, UNIT, d), lambda s, me: (layer, start + s, 0))
    specs = [wide, wide, tall] * 3
    if len(grads) == n:
        grad = pl.BlockSpec((2, 3) + grads[0].shape[2:], lambda s, me: (0, s, 0, 0))
    else:
        grad = pl.BlockSpec((3,) + grads[0].shape[1:], lambda s, me: (s, 0, 0))
    held = [] if done is None else list(done)
    count = len(grads)
    return pl.pallas_call(
        functools.partial(adamw_kernel, n, count),
        grid_spec=pltpu.PrefetchScalarGridSpec(
            num_scalar_prefetch=1,
            grid=(units,),
            in_specs=[pl.BlockSpec(factor.shape, lambda s, me: (0, 0))]
            + [grad] * count
            + specs
            + [pl.BlockSpec(memory_space=pl.ANY)] * len(held),
            out_specs=specs,
        ),
        out_shape=[jax.ShapeDtypeStruct(a.shape, a.dtype) for a in arrays],
        input_output_aliases={2 + count + 9 + i: i for i in range(len(held))},
        compiler_params=params(dimension_semantics=("arbitrary",)),
        cost_estimate=pl.CostEstimate(flops=10**9 * 4 * units, bytes_accessed=22 * 3 * units * UNIT * d, transcendentals=0),
    )(me[None], factor, *grads, *arrays, *held)


def tie(value, *others):
    return lax.optimization_barrier((value, *others))[0]


def solution(mesh):
    n = mesh.shape["dp"]

    def step(x, dy, *arrays):
        weights = arrays[:3]
        wg, wu, wd = weights
        x, dy = x[0], dy[0]
        me = lax.axis_index("dp")
        count = sum(a.size for a in weights)

        def send(array, by):
            return lax.ppermute(array, "dp", [(i, (i + by) % n) for i in range(n)])

        def spread(a, b):
            ra, lb = send(a, 1), send(b, -1)
            rb, la = send(b, 1), send(a, -1)
            return a, b, la, lb, ra, rb

        def onward(got):
            a, b, la, lb, ra, rb = got
            return a, b, la, lb, send(ra, 1), send(lb, -1), ra, rb

        starts = {(layer, i): sum(PIECES[layer][:i]) for layer in PIECES for i in range(len(PIECES[layer]))}
        A, B, C, D, E, F = starts

        def make(key, a, by_h, kept=(), tasks=(), number=0):
            units = PIECES[key[0]][key[1]]
            return piece(a, by_h, weights, kept, key[0], starts[key], units, n, tasks, number)

        a0, h1, a1, gate, up = forward(x, wg, wu, wd, 0)
        (*pa, da), = make(A, a1, dy)
        (*pb, db), (sa, qa) = make(B, a1, dy, (), [Sum(pa, n, 3)], 1)
        (*pc, dc), (sb, qb), ga = make(C, a1, dy, (), [Sum(pb, n, 2), Gather(sa, n, 4)], 2)
        (by_h,), (sc, qc) = back((da, db, dc), wg, wu, h1, dy, 1, n, [Sum(pc, n, 3)], 3)
        pd, gb, gc = make(D, a0, by_h, (gate, up), [Gather(sb, n, 3), Gather(sc, n, 7)], 4)
        pe, (sd, qd) = make(E, a0, by_h, (gate, up), [Sum(pd, n, 3)], 5)
        pf, (se, qe) = make(F, a0, by_h, (gate, up), [Sum(pe, n, 3)], 6)
        sf, _, factor = finish(pf, n, (qa, qb, qc, qd, qe), count, 7)

        got = {D: spread(tie(sd[0], factor), sd[1]), E: spread(tie(se[0], factor), se[1]), F: spread(sf[0], sf[1])}
        step_on = lambda key, done, grads: adamw(arrays, done, grads, me, factor, key[0], starts[key], n)
        done = step_on(A, None, (sa, *ga))
        done = step_on(B, done, (sb, *gb))
        done = step_on(C, done, (sc, *gc))
        for key in (D, E, F):
            done = step_on(key, done, onward(got[key]))
        return tuple(done)

    return jax.shard_map(
        step,
        mesh=mesh,
        in_specs=(P(("rep", "dp"), None, None),) * 2 + (P(None, None, None),) * 9,
        out_specs=(P("rep", None, None),) * 9,
        check_vma=False,
    )
```

```python
import functools

import jax
import jax.numpy as jnp
from jax import lax
from jax.experimental import pallas as pl
from jax.experimental.pallas import tpu as pltpu
from jax.sharding import PartitionSpec as P


F32, BF16 = jnp.float32, jnp.bfloat16
TILE = 512
LONG = 1024
SUB = 512
UNIT = 256
FULL_VMEM = 60 << 20
GROUPS = {1: ((0, 2), (2, 4), (4, 6)), 0: ((0, 3), (3, 6))}


def params(**kw):
    return pltpu.CompilerParams(vmem_limit_bytes=FULL_VMEM, **kw)


def cost(matmuls, moved, tokens, d, width):
    return pl.CostEstimate(flops=2 * matmuls * tokens * d * width, bytes_accessed=moved, transcendentals=0)


def dot(a, b, ca, cb):
    return lax.dot_general(a, b, (((ca,), (cb,)), ((), ())), preferred_element_type=F32)


def scale_of(wide):
    return lax.rsqrt(jnp.mean(wide * wide, -1, keepdims=True) + 1e-6)


def forward_kernel(x_ref, wg_ref, wu_ref, wd_ref, a_ref, h_ref, b_ref, gate_ref, up_ref, p_ref):
    rows = SUB
    for sub in range(x_ref.shape[0] // SUB):
        at = slice(sub * rows, (sub + 1) * rows)
        x = x_ref[at, :].astype(F32)
        a = (x * scale_of(x)).astype(BF16)
        a_ref[at, :] = a
        for j in range(p_ref.shape[1] // UNIT):
            cols = slice(j * UNIT, (j + 1) * UNIT)
            gate = dot(a, wg_ref[:, cols], 1, 0)
            up = dot(a, wu_ref[:, cols], 1, 0)
            gate_ref[at, cols] = gate
            up_ref[at, cols] = up
            p_ref[at, cols] = (gate * jax.nn.sigmoid(gate) * up).astype(BF16)
    for sub in range(x_ref.shape[0] // SUB):
        at = slice(sub * rows, (sub + 1) * rows)
        h = x_ref[at, :] + dot(p_ref[at, :], wd_ref[...], 1, 0).astype(BF16)
        h_ref[at, :] = h
        wide = h.astype(F32)
        b_ref[at, :] = (wide * scale_of(wide)).astype(BF16)


def forward(x, wg, wu, wd, layer):
    tokens, d = x.shape
    ff = wg.shape[2]
    rows = pl.BlockSpec((TILE, d), lambda t: (t, 0))
    hidden = pl.BlockSpec((TILE, ff), lambda t: (t, 0))
    whole = lambda r, c: pl.BlockSpec((None, r, c), lambda t: (layer, 0, 0), pipeline_mode=pl.Buffered(1))
    out = jax.ShapeDtypeStruct((tokens, d), BF16)
    wide = jax.ShapeDtypeStruct((tokens, ff), F32)
    return pl.pallas_call(
        forward_kernel,
        grid=(tokens // TILE,),
        in_specs=[rows, whole(d, ff), whole(d, ff), whole(ff, d)],
        out_specs=[rows] * 3 + [hidden] * 2,
        out_shape=[out] * 3 + [wide] * 2,
        scratch_shapes=[pltpu.VMEM((TILE, ff), BF16)],
        compiler_params=params(dimension_semantics=("arbitrary",)),
        cost_estimate=cost(3, 8 * tokens * d + 6 * d * ff, tokens, d, ff),
        name="forward",
    )(x, wg, wu, wd)


def remote(src, dst, sems, i, to):
    send, recv = sems
    return pltpu.make_async_remote_copy(
        src_ref=src, dst_ref=dst, send_sem=send.at[i], recv_sem=recv.at[i], device_id={"dp": to}, device_id_type=pl.DeviceIdType.MESH
    )


def around(n):
    me = lax.axis_index("dp")
    return lax.rem(me + 1, n), lax.rem(me + n - 1, n)


class Sum:
    def __init__(self, parts, n, middle):
        self.operands, self.n, self.middle = list(parts), n, middle
        half = parts[0].shape[1:]
        self.half = half
        self.outs = [jax.ShapeDtypeStruct(half, BF16)] * 2 + [jax.ShapeDtypeStruct((8, half[-1]), F32)]
        self.out_specs = [pl.BlockSpec(half, lambda t: (0,) * 3)] * 2 + [pl.BlockSpec((8, half[-1]), lambda t: (0, 0))]
        self.scratch = [pltpu.VMEM((k, *half), BF16) for k in (2, 2, 4, 2, 2)]
        self.scratch += [pltpu.SemaphoreType.DMA((6,)), pltpu.SemaphoreType.DMA((6,)), pltpu.SemaphoreType.DMA((1,))]

    def bind(self, refs):
        to_right, to_left, rest, share_a, share_b, self.squares, self.from_left, self.from_right, self.rest, self.sums, self.second, *sems, local = refs
        self.share = share_a, share_b
        right, left = around(self.n)
        self.copies = [
            remote(to_right.at[0], self.from_left.at[0], sems, 0, right),
            remote(to_left.at[0], self.from_right.at[0], sems, 1, left),
            remote(to_right.at[1], self.from_left.at[1], sems, 2, right),
            remote(to_left.at[1], self.from_right.at[1], sems, 3, left),
            remote(self.sums.at[0], self.second.at[0], sems, 4, right),
            remote(self.sums.at[1], self.second.at[1], sems, 5, left),
        ]
        self.local = pltpu.make_async_copy(rest, self.rest, local.at[0])

    def start(self):
        self.local.start()
        for copy in self.copies[:4]:
            copy.start()

    def step(self):
        self.local.wait()
        for i, came in enumerate((self.from_left, self.from_right)):
            self.copies[i].wait_recv()

            @pl.loop(0, self.half[0])
            def _(k):
                self.sums[i, k] = (self.rest[i, k].astype(F32) + came[0, k].astype(F32)).astype(BF16)

            self.copies[4 + i].start()

    def end(self):
        for copy in self.copies[2:]:
            copy.wait_recv()
        self.squares[...] = jnp.zeros_like(self.squares)
        for i, came in enumerate((self.from_right, self.from_left)):

            @pl.loop(0, self.half[0])
            def _(k):
                whole = self.rest[2 + i, k].astype(F32) + came[1, k].astype(F32) + self.second[i, k].astype(F32)
                self.share[i][k] = whole.astype(BF16)
                rounded = whole.astype(BF16).astype(F32)
                self.squares[...] += jnp.sum((rounded * rounded).reshape(-1, 8, rounded.shape[-1]), 0)

        for copy in self.copies:
            copy.wait_send()


def gather_copies(a, b, to, sems, base, n):
    right, left = around(n)
    after_a, after_b, far_a, far_b, before_a, before_b = to
    return [
        remote(a, before_a, sems, base, right),
        remote(b, after_b, sems, base + 1, left),
        remote(b, before_b, sems, base + 2, right),
        remote(a, after_a, sems, base + 3, left),
        remote(before_a, far_a, sems, base + 4, right),
        remote(after_b, far_b, sems, base + 5, left),
    ]


def start_gather(copies):
    for copy in copies[:4]:
        copy.start()


def pass_on(copies):
    for i in range(2):
        copies[i].wait_recv()
        copies[4 + i].start()


def end_gather(copies):
    for copy in copies[2:]:
        copy.wait_recv()
    for copy in copies:
        copy.wait_send()


class Gather:
    def __init__(self, halves, n, middle):
        self.operands, self.n, self.middle = list(halves), n, middle
        self.outs = [jax.ShapeDtypeStruct(halves[0].shape, BF16)] * 6
        self.out_specs = [pl.BlockSpec(memory_space=pl.ANY)] * 6
        self.scratch = [pltpu.SemaphoreType.DMA((6,)), pltpu.SemaphoreType.DMA((6,))]

    def bind(self, refs):
        self.copies = gather_copies(*refs[:2], refs[2:8], refs[8:], 0, self.n)

    def start(self):
        start_gather(self.copies)

    def step(self):
        pass_on(self.copies)

    def end(self):
        end_gather(self.copies)


def run(body, n, steps, ins, in_specs, outs, out_specs, scratch, tasks, number, **kw):
    groups = [(ins, outs, scratch), *((t.operands, t.outs, t.scratch) for t in tasks)]

    def kernel(*refs):
        at, dealt = 0, [[] for _ in groups]
        for which in range(3):
            for i, group in enumerate(groups):
                dealt[i] += refs[at : at + len(group[which])]
                at += len(group[which])
        t = pl.program_id(0)
        for task, own in zip(tasks, dealt[1:], strict=True):
            task.bind(own)
        if tasks:

            @pl.when(t == 0)
            def _():
                barrier = pltpu.get_barrier_semaphore()
                for to in around(n):
                    pl.semaphore_signal(barrier, inc=1, device_id={"dp": to}, device_id_type=pl.DeviceIdType.MESH)
                pl.semaphore_wait(barrier, 2)
                for task in tasks:
                    task.start()

            for task in tasks:
                pl.when(t == task.middle)(task.step)
        body(*dealt[0])
        for task in tasks:
            pl.when(t == steps - 1)(task.end)

    anywhere = pl.BlockSpec(memory_space=pl.ANY)
    out = pl.pallas_call(
        kernel,
        grid=(steps,),
        in_specs=list(in_specs) + [anywhere for t in tasks for _ in t.operands],
        out_specs=list(out_specs) + [s for t in tasks for s in t.out_specs],
        out_shape=list(outs) + [o for t in tasks for o in t.outs],
        scratch_shapes=list(scratch) + [s for t in tasks for s in t.scratch],
        compiler_params=params(
            dimension_semantics=("arbitrary",), **(dict(collective_id=number, has_side_effects=True) if tasks else {})
        ),
        **kw,
    )(*ins, *(o for t in tasks for o in t.operands))
    out, given = list(out), []
    own, out = out[: len(outs)], out[len(outs) :]
    for t in tasks:
        given.append(out[: len(t.outs)])
        out = out[len(t.outs) :]
    return own, *given


def layer_kernel(plan, n, saved, *refs):
    groups, gathers, sources = plan
    refs = list(refs)
    take = lambda k: [refs.pop(0) for _ in range(k)]
    a_ref, dy_ref = take(2)
    gate_ref, up_ref = take(2)
    (wd_ref,) = take(1)
    given = [take(2) for _ in range(sources)]
    last = take(3)
    dgate_ref, dup_ref = take(0 if saved else 2) or (None, None)
    shares = [take(2) for _ in groups]
    (squares,) = take(1)
    places = [take(6) for _ in range(len({g for g, *_ in gathers}))]
    acc, acc_d, p_s = take(3)
    if saved:
        dgate_ref, dup_ref = take(2)
    to_right, to_left, rest, from_left, from_right, sums, second, *sems = refs
    sum_sems, gather_sems = sems[:2], sems[2:]
    p, t = pl.program_id(0), pl.program_id(1)
    parts, steps = pl.num_programs(0), pl.num_programs(1)
    now = p * steps + t
    right, left = around(n)
    _, _, three, part, _ = to_right.shape

    def hops(q):
        base = q * 6
        return [
            remote(to_right.at[q, 0], from_left.at[q, 0], sum_sems, base, right),
            remote(to_left.at[q, 0], from_right.at[q, 0], sum_sems, base + 1, left),
            remote(to_right.at[q, 1], from_left.at[q, 1], sum_sems, base + 2, right),
            remote(to_left.at[q, 1], from_right.at[q, 1], sum_sems, base + 3, left),
            remote(sums.at[q, 0], second.at[q, 0], sum_sems, base + 4, right),
            remote(sums.at[q, 1], second.at[q, 1], sum_sems, base + 5, left),
        ]

    def second_hop(q):
        copies = hops(q)
        for i, came in enumerate((from_left, from_right)):
            copies[i].wait_recv()

            @pl.loop(0, three)
            def _(k):
                sums[q, i, k] = (rest[q, i, k].astype(F32) + came[q, 0, k].astype(F32)).astype(BF16)

            copies[4 + i].start()

    def end_sum(q):
        copies = hops(q)
        for copy in copies[2:]:
            copy.wait_recv()
        for (low, high), share in zip(groups, shares, strict=True):

            @pl.when((q >= low) & (q < high))
            def _():
                for i, came in enumerate((from_right, from_left)):

                    @pl.loop(0, three)
                    def _(k):
                        whole = rest[q, 2 + i, k].astype(F32) + came[q, 1, k].astype(F32) + second[q, i, k].astype(F32)
                        share[i][(q - low) * three + k] = whole.astype(BF16)
                        rounded = whole.astype(BF16).astype(F32)
                        squares[...] += jnp.sum((rounded * rounded).reshape(-1, 8, rounded.shape[-1]), 0)

        for copy in copies:
            copy.wait_send()

    moves = []
    order = sorted({g for g, *_ in gathers})
    for number, (g, unit, first, then) in enumerate(gathers):
        own = given[g - len(groups)] if g >= len(groups) else shares[g]
        rows = pl.ds(unit * three, three)
        to = [ref.at[rows] for ref in places[order.index(g)]]
        moves.append((first, then, gather_copies(own[0].at[rows], own[1].at[rows], to, gather_sems, 6 * number, n)))

    @pl.when(now == 0)
    def _():
        squares[...] = jnp.zeros_like(squares)
        barrier = pltpu.get_barrier_semaphore()
        for to in around(n):
            pl.semaphore_signal(barrier, inc=1, device_id={"dp": to}, device_id_type=pl.DeviceIdType.MESH)
        pl.semaphore_wait(barrier, 2)

    @pl.when((t == 0) & (p > 0))
    def _():
        for copy in hops(p - 1)[:4]:
            copy.start()

    for first, then, copies in moves:
        pl.when(now == first)(functools.partial(start_gather, copies))
        pl.when(now == then)(functools.partial(pass_on, copies))

    @pl.when((t == steps - 1) & (p > 0))
    def _():
        second_hop(p - 1)

    @pl.when((t == steps - 1) & (p > 1))
    def _():
        end_sum(p - 2)

    @pl.when(t == 0)
    def _():
        acc[...] = jnp.zeros_like(acc)
        acc_d[...] = jnp.zeros_like(acc_d)

    def accumulate(at):
        acc[:, :UNIT] += dot(a_ref[at, :], dgate_ref[at, :], 0, 0)
        acc[:, UNIT:] += dot(a_ref[at, :], dup_ref[at, :], 0, 0)
        acc_d[...] += dot(p_s[at, :], dy_ref[at, :], 0, 0)

    spans = [slice(low, low + SUB) for low in range(0, a_ref.shape[0], SUB)]
    for number, at in enumerate(spans):
        gate = gate_ref[at, :] if saved else dot(a_ref[at, :], gate_ref[...], 1, 0)
        up = up_ref[at, :] if saved else dot(a_ref[at, :], up_ref[...], 1, 0)
        dp = dot(dy_ref[at, :], wd_ref[...], 1, 1).astype(BF16).astype(F32)
        s = jax.nn.sigmoid(gate)
        act = gate * s
        p_s[at, :] = (act * up).astype(BF16)
        dup_ref[at, :] = (dp * act).astype(BF16)
        dgate_ref[at, :] = (dp * up * (s * (1.0 + gate * (1.0 - s)))).astype(BF16)
        if number:
            accumulate(spans[number - 1])
    accumulate(spans[-1])

    me = lax.axis_index("dp")
    small = UNIT // (2 * n)

    def put(ref, by, half):
        at = lax.rem(me + by, n) * 2 + half
        rows = pl.ds(pl.multiple_of(at * part, part), part)
        thin = pl.ds(pl.multiple_of(at * small, small), small)
        ref[0] = acc[rows, :UNIT].astype(BF16)
        ref[1] = acc[rows, UNIT:].astype(BF16)
        for b in range(part // small):
            ref[2, b * small : (b + 1) * small, :] = acc_d[thin, b * UNIT : (b + 1) * UNIT].astype(BF16)

    def put_all(to_right, to_left, rest):
        put(to_right.at[0], 2, 0)
        put(to_right.at[1], 1, 1)
        put(to_left.at[0], 2, 1)
        put(to_left.at[1], n - 1, 0)
        put(rest.at[0], 1, 0)
        put(rest.at[1], n - 1, 1)
        put(rest.at[2], 0, 0)
        put(rest.at[3], 0, 1)

    @pl.when((t == steps - 1) & (p < parts - 1))
    def _():
        put_all(to_right.at[p], to_left.at[p], rest.at[p])

    @pl.when((t == steps - 1) & (p == parts - 1))
    def _():
        put_all(*last)
        end_sum(p - 1)
        for _, _, copies in moves:
            end_gather(copies)


def layer_step(a, dy, weights, saved, layer, n, given, gathers, number):
    tokens, d = a.shape
    ff = weights[0].shape[2]
    groups = GROUPS[layer]
    parts, tile, part = ff // UNIT, LONG, d // (2 * n)
    half = (3, part, UNIT)
    rows = pl.BlockSpec((tile, d), lambda p, t: (t, 0))
    cols = pl.BlockSpec((None, d, UNIT), lambda p, t: (layer, 0, p))
    down = pl.BlockSpec((None, UNIT, d), lambda p, t: (layer, p, 0))
    hidden = pl.BlockSpec((tile, UNIT), lambda p, t: (t, p))
    anywhere = pl.BlockSpec(memory_space=pl.ANY)
    const = lambda shape: pl.BlockSpec(shape, lambda p, t: (0,) * len(shape))
    like = lambda shape, dtype=BF16: jax.ShapeDtypeStruct(shape, dtype)
    shapes = [(2, *half), (2, *half), (4, *half)]
    outs = [(like(s), const(s)) for s in shapes]
    if not saved:
        outs += [(like((tokens, ff)), hidden)] * 2
    kept = [(3 * (high - low), part, UNIT) for low, high in groups]
    for s in kept:
        outs += [(like(s), const(s))] * 2
    outs.append((like((8, UNIT), F32), const((8, UNIT))))
    brought = sorted({g for g, *_ in gathers})
    for g in brought:
        s = kept[g] if g < len(groups) else given[g - len(groups)][0].shape
        outs += [(like(s), anywhere)] * 6
    busy = parts - 1
    scratch = [pltpu.VMEM((d, 2 * UNIT), F32), pltpu.VMEM((UNIT, d), F32), pltpu.VMEM((tile, UNIT), BF16)]
    if saved:
        scratch += [pltpu.VMEM((tile, UNIT), BF16)] * 2
    scratch += [pltpu.VMEM((busy, k, *half), BF16) for k in (2, 2, 4, 2, 2, 2, 2)]
    scratch += [pltpu.SemaphoreType.DMA((6 * busy,))] * 2 + [pltpu.SemaphoreType.DMA((6 * len(gathers),))] * 2
    out = pl.pallas_call(
        functools.partial(layer_kernel, (groups, gathers, len(given)), n, bool(saved)),
        grid=(parts, tokens // tile),
        in_specs=[rows, rows] + [hidden if saved else cols] * 2 + [down] + [anywhere] * (2 * len(given)),
        out_specs=[spec for _, spec in outs],
        out_shape=[shape for shape, _ in outs],
        scratch_shapes=scratch,
        compiler_params=params(dimension_semantics=("arbitrary", "arbitrary"), collective_id=number, has_side_effects=True),
        cost_estimate=cost(4 if saved else 6, 4 * tokens * d + 12 * d * ff, tokens, d, ff),
    )(a, dy, *(saved or weights[:2]), weights[2], *(h for g in given for h in g))
    out = list(out)
    take = lambda k: [out.pop(0) for _ in range(k)]
    return take(3), take(0 if saved else 2), [take(2) for _ in groups], take(1)[0], [take(6) for _ in brought]


def back_kernel(dgate_ref, dup_ref, wg_ref, wu_ref, h_ref, dy_ref, out_ref):
    for low in range(0, h_ref.shape[0], SUB):
        span = slice(low, low + SUB)
        by_gate = dot(dgate_ref[span, :], wg_ref[...], 1, 1).astype(BF16)
        da = (by_gate + dot(dup_ref[span, :], wu_ref[...], 1, 1).astype(BF16)).astype(F32)
        h = h_ref[span, :].astype(F32)
        scale = scale_of(h)
        along = jnp.mean(da * h, -1, keepdims=True)
        out_ref[span, :] = dy_ref[span, :] + (da * scale - h * (scale * scale * scale * along)).astype(BF16)


def back(dgate, dup, wg, wu, h, dy, layer, n, tasks=(), number=0):
    tokens, d = h.shape
    ff = wg.shape[2]
    rows = pl.BlockSpec((TILE, d), lambda t: (t, 0))
    whole = pl.BlockSpec((None, d, ff), lambda t: (layer, 0, 0), pipeline_mode=pl.Buffered(1))
    hidden = pl.BlockSpec((TILE, ff), lambda t: (t, 0))
    return run(
        back_kernel,
        n,
        tokens // TILE,
        (dgate, dup, wg, wu, h, dy),
        [hidden, hidden, whole, whole, rows, rows],
        [jax.ShapeDtypeStruct((tokens, d), BF16)],
        [rows],
        (),
        tasks,
        number,
        cost_estimate=cost(2, 6 * tokens * d + 4 * d * ff + 4 * tokens * ff, tokens, d, ff),
        name="back",
    )


class Finish(Sum):
    def __init__(self, parts, n, others, count):
        super().__init__(parts, n, 0)
        self.operands, self.count, self.others = self.operands + list(others), count, len(others)
        tile = (8, others[0].shape[1])
        self.outs.append(jax.ShapeDtypeStruct(tile, F32))
        self.out_specs.append(pl.BlockSpec(tile, lambda t: (0, 0)))
        self.scratch += [pltpu.VMEM((n, *tile), F32), pltpu.VMEM((len(others), *tile), F32), pltpu.SemaphoreType.DMA((1,))]
        self.scratch += [pltpu.SemaphoreType.DMA((n,)), pltpu.SemaphoreType.DMA((n,))]


def finish_kernel(task, refs):
    k = task.others
    parts, others, share, squares, factor = refs[:3], refs[3 : 3 + k], refs[3 + k : 5 + k], refs[5 + k], refs[6 + k]
    rest = refs[7 + k :]
    terms, held, local, send, recv = rest[8:]
    n = task.n
    me = lax.axis_index("dp")
    barrier = pltpu.get_barrier_semaphore()
    for by in range(1, n):
        pl.semaphore_signal(barrier, inc=1, device_id={"dp": lax.rem(me + by, n)}, device_id_type=pl.DeviceIdType.MESH)
    pl.semaphore_wait(barrier, n - 1)
    task.bind([*parts, *share, squares, *rest[:8]])
    task.start()
    for i, other in enumerate(others):
        copy = pltpu.make_async_copy(other, held.at[i], local.at[0])
        copy.start()
        copy.wait()
    task.step()
    task.end()
    total = squares[...]
    for i in range(k):
        total += held[i]
    terms[me] = total
    copies = [remote(terms.at[me], terms.at[me], (send, recv), by, lax.rem(me + by, n)) for by in range(1, n)]
    for copy in copies:
        copy.start()
    for by in range(1, n):
        sender = lax.rem(me + n - by, n)
        remote(terms.at[sender], terms.at[sender], (send, recv), by, lax.rem(me + by, n)).wait_recv()
    everything = terms[0]
    for i in range(1, n):
        everything += terms[i]
    everything = jnp.sum(jnp.sum(everything, 0, keepdims=True), 1, keepdims=True)
    factor[...] = jnp.broadcast_to(jnp.minimum(1.0, 0.5 * lax.rsqrt(everything / task.count + 1e-30)), factor.shape)
    for copy in copies:
        copy.wait_send()


def finish(parts, n, others, count, number):
    task = Finish(parts, n, others, count)
    anywhere = pl.BlockSpec(memory_space=pl.ANY)
    return pl.pallas_call(
        lambda *refs: finish_kernel(task, refs),
        grid=(1,),
        in_specs=[anywhere] * len(task.operands),
        out_specs=task.out_specs,
        out_shape=task.outs,
        scratch_shapes=task.scratch,
        compiler_params=params(collective_id=number, has_side_effects=True),
        cost_estimate=pl.CostEstimate(flops=4 * 10**9, bytes_accessed=10**6, transcendentals=0),
        name="finish",
    )(*task.operands)


def adamw_kernel(n, spans, me_ref, factor_ref, *refs):
    grads, ins, outs = refs[: 2 * n * len(spans)], refs[2 * n * len(spans) :][:9], refs[-9:]
    factor = factor_ref[0:1, 0:1]
    me = me_ref[0]

    def take(grads):
        for number, ref in enumerate(grads):
            at = lax.rem(me + number // 2, n) * 2 + number % 2
            part = ref.shape[1]
            for which in range(3):
                w_ref, m_ref, v_ref = (ins[which + 3 * i] for i in range(3))
                w_out, m_out, v_out = (outs[which + 3 * i] for i in range(3))
                if which < 2:
                    spots = [((pl.ds(pl.multiple_of(at * part, part), part), slice(None)), ref[which])]
                else:
                    small = w_ref.shape[0] // (2 * n)
                    rows = pl.ds(pl.multiple_of(at * small, small), small)
                    spots = [((rows, slice(b * UNIT, (b + 1) * UNIT)), ref[which, b * small : (b + 1) * small]) for b in range(part // small)]
                for spot, g in spots:
                    g = g.astype(F32) * factor
                    m = 0.9 * m_ref[spot] + 0.1 * g
                    v = 0.95 * v_ref[spot] + 0.05 * g * g
                    w = w_ref[spot].astype(F32)
                    m_out[spot] = m
                    v_out[spot] = v
                    w_out[spot] = (w - 0.02 * (m * lax.rsqrt(v + 1e-8) + 0.1 * w)).astype(BF16)

    s = pl.program_id(0)
    for i, (low, high) in enumerate(spans):
        pl.when((s >= low) & (s < high))(functools.partial(take, grads[2 * n * i : 2 * n * (i + 1)]))


def adamw(arrays, done, groups, me, factor, layer, start, n):
    d = arrays[0].shape[1]
    ends = [0]
    for group in groups:
        ends.append(ends[-1] + group[0].shape[0] // 3)
    spans = list(zip(ends, ends[1:]))
    wide = pl.BlockSpec((None, d, UNIT), lambda s, me: (layer, 0, start + s))
    tall = pl.BlockSpec((None, UNIT, d), lambda s, me: (layer, start + s, 0))
    specs = [wide, wide, tall] * 3
    grad = lambda low, high, g: pl.BlockSpec((3,) + g.shape[1:], lambda s, me: (jnp.clip(s - low, 0, high - low - 1), 0, 0))
    grads = [(g, grad(*span, g)) for group, span in zip(groups, spans, strict=True) for g in group]
    held = [] if done is None else list(done)
    return pl.pallas_call(
        functools.partial(adamw_kernel, n, spans),
        grid_spec=pltpu.PrefetchScalarGridSpec(
            num_scalar_prefetch=1,
            grid=(ends[-1],),
            in_specs=[pl.BlockSpec(factor.shape, lambda s, me: (0, 0))]
            + [spec for _, spec in grads]
            + specs
            + [pl.BlockSpec(memory_space=pl.ANY)] * len(held),
            out_specs=specs,
        ),
        out_shape=[jax.ShapeDtypeStruct(a.shape, a.dtype) for a in arrays],
        input_output_aliases={2 + len(grads) + 9 + i: i for i in range(len(held))},
        compiler_params=params(dimension_semantics=("arbitrary",)),
        cost_estimate=pl.CostEstimate(flops=10**9 * 4 * ends[-1], bytes_accessed=22 * 3 * ends[-1] * UNIT * d, transcendentals=0),
    )(me[None], factor, *(g for g, _ in grads), *arrays, *held)


def tie(value, *others):
    return lax.optimization_barrier((value, *others))[0]


def solution(mesh):
    n = mesh.shape["dp"]

    def step(x, dy, *arrays):
        weights = arrays[:3]
        wg, wu, wd = weights
        x, dy = x[0], dy[0]
        me = lax.axis_index("dp")
        count = sum(a.size for a in weights)

        def send(array, by):
            return lax.ppermute(array, "dp", [(i, (i + by) % n) for i in range(n)])

        def spread(a, b):
            ra, lb = send(a, 1), send(b, -1)
            rb, la = send(b, 1), send(a, -1)
            return a, b, la, lb, ra, rb

        def onward(got):
            a, b, la, lb, ra, rb = got
            return a, b, la, lb, send(ra, 1), send(lb, -1), ra, rb

        a0, h1, a1, gate, up = forward(x, wg, wu, wd, 0)
        last, by_hidden, shares, squares, (first,) = layer_step(a1, dy, weights, (), 1, n, (), ((0, 0, 13, 17), (0, 1, 17, 21)), 1)
        tasks = [Sum(last, n, 2), Gather(shares[1], n, 4)]
        (by_h,), own, second = back(*by_hidden, wg, wu, h1, dy, 1, n, tasks, 2)
        own, fresh = own[:2], own[2]
        waiting = ((2, 0, 0, 3), (2, 1, 1, 5), (3, 0, 2, 7))
        last, _, ours, sums, (third, fourth) = layer_step(a0, by_h, weights, (gate, up), 0, n, (shares[2], own), waiting, 3)
        sa, sb, _, factor = finish(last, n, (squares, fresh, sums), count, 4)

        got = [spread(*[tie(h, factor) for h in ours[0]]), spread(*[tie(h, factor) for h in ours[1]]), spread(sa, sb)]
        one = [(*shares[0], *first), (*shares[1], *second), (*shares[2], *third), (*own, *fourth)]
        step_on = lambda done, groups, layer, start: adamw(arrays, done, groups, me, factor, layer, start, n)
        done = step_on(None, one[:2], 1, 0)
        done = step_on(done, one[2:], 1, GROUPS[1][2][0])
        done = step_on(done, [onward(got[0])], 0, 0)
        done = step_on(done, [onward(got[2])], 0, GROUPS[0][-1][1])
        done = step_on(done, [onward(got[1])], 0, GROUPS[0][1][0])
        return tuple(done)

    return jax.shard_map(
        step,
        mesh=mesh,
        in_specs=(P(("rep", "dp"), None, None),) * 2 + (P(None, None, None),) * 9,
        out_specs=(P("rep", None, None),) * 9,
        check_vma=False,
    )
```
